32 devices in a mesh: seq: 16 (over z, y, x), head: 2 (over core).
Axes of the slice: x: 2, y: 2, z: 4, core: 2. Of those that a mesh axis runs over, the one named last changes fastest.
Arguments:
- queries: bfloat16 [32768, 1024], P('seq', 'head'), may hold values from -10 to 10
- key_vectors: bfloat16 [32768, 1024], P('seq', 'head'), may hold values from -10 to 10
- value_vectors: bfloat16 [32768, 1024], P('seq', 'head'), may hold values from -6 to 6
- grad_output: bfloat16 [32768, 1024], P('seq', 'head'), may hold values from -6 to 6
Outputs:
- attended: bfloat16 [32768, 1024], P('seq', 'head')
- grad_queries: bfloat16 [32768, 1024], P('seq', 'head')
- grad_keys: bfloat16 [32768, 1024], P('seq', 'head')
- grad_values: bfloat16 [32768, 1024], P('seq', 'head')
The draws below stay inside these ranges and needn't reach their ends.
All inputs are finite; a program needn't handle non-finite values.
Results may differ from the reference program's by a relative error of at most 0.019.
Values may be sent and summed in bfloat16 or wider, within the bound.
A program may use at most 128 MiB of HBM per device.

```python
import math
import jax
import jax.numpy as jnp
from jax import lax

ROW_LEN = 512
HEADS = 8
HEAD_DIM = 128
ROWS = 64
TOKENS = 32768


def draw_pair(key):
    base = jax.random.fold_in(key, 11)
    draw_keys = jax.random.split(base, 2)
    width = HEADS * HEAD_DIM
    query_grid = jnp.clip(jax.random.normal(draw_keys[0], (ROWS, ROW_LEN, width), jnp.float32), -6.0, 6.0)
    key_grid = jnp.clip(jax.random.normal(draw_keys[1], (ROWS, ROW_LEN, width), jnp.float32), -6.0, 6.0)
    return (query_grid.reshape(TOKENS, width), key_grid.reshape(TOKENS, width))


def draw_queries(key, part):
    return draw_pair(key)[0].astype(jnp.bfloat16)


def draw_key_vectors(key, part):
    return draw_pair(key)[1].astype(jnp.bfloat16)


def shard_levels(rng, extent, shards, least, top_value):
    loudness, own = 1.0, jax.random.fold_in(rng, 6)
    for dim, parts in shards:
        draws = jnp.exp(jax.random.uniform(jax.random.fold_in(own, dim), (parts,), jnp.float32, least / len(shards), top_value / len(shards)))
        loudness = loudness * jnp.repeat(draws, extent[dim] // parts).reshape([-1 if axis == dim else 1 for axis in range(len(extent))])
    return loudness


def bell_draw(stream_key, dims, scale, bound, cuts=(), dtype=jnp.bfloat16):
    entries = scale * jax.random.normal(stream_key, dims, jnp.float32)
    if cuts:
        entries = entries * shard_levels(stream_key, dims, cuts, -0.22, 0.18)
    return jnp.clip(entries, -bound, bound).astype(dtype)


def setup_inputs(seed: int = 0) -> dict:
    arg_keys = jax.random.split(jax.random.key(seed), 5)
    queries = draw_queries(jax.random.fold_in(arg_keys[4], 71), 0)
    key_vectors = draw_key_vectors(jax.random.fold_in(arg_keys[4], 71), 0)
    value_vectors = bell_draw(arg_keys[2], (TOKENS, HEADS * HEAD_DIM), 1.0, 6.0, ((0, 16), (1, 2)))
    grad_output = bell_draw(arg_keys[3], (TOKENS, HEADS * HEAD_DIM), 1.0, 6.0, ((0, 16), (1, 2)))
    return {"queries": queries, "key_vectors": key_vectors, "value_vectors": value_vectors, "grad_output": grad_output}


NEG_FILL = -1e+30

def rounded(array):
    return lax.optimization_barrier(array.astype(jnp.bfloat16)).astype(jnp.float32)

def pattern_forward(query_block, key_block, value_block, allowed):
    scaling = 1.0 / math.sqrt(HEAD_DIM)
    scores = jnp.einsum('qhd,khd->hqk', query_block.astype(jnp.float32), key_block.astype(jnp.float32)) * scaling
    maxima = lax.optimization_barrier(jnp.max(jnp.where(allowed, scores, NEG_FILL), axis=-1))
    weights = jnp.where(allowed, jnp.exp(scores - maxima[..., None]), 0.0)
    totals = lax.optimization_barrier(jnp.sum(weights, axis=-1))
    accumulated = jnp.einsum('hqk,khd->qhd', rounded(weights), value_block.astype(jnp.float32))
    return (accumulated, maxima.T, totals.T)

def pattern_backward(query_block, key_block, value_block, grad_block, log_totals, correction, allowed):
    scaling = 1.0 / math.sqrt(HEAD_DIM)
    query_f = query_block.astype(jnp.float32)
    key_f = key_block.astype(jnp.float32)
    grad_f = grad_block.astype(jnp.float32)
    scores = jnp.einsum('qhd,khd->hqk', query_f, key_f) * scaling
    probabilities = jnp.where(allowed, jnp.exp(scores - log_totals.T[..., None]), 0.0)
    grad_value = jnp.einsum('hqk,qhd->khd', rounded(probabilities), grad_f)
    grad_probs = jnp.einsum('qhd,khd->hqk', grad_f, value_block.astype(jnp.float32))
    grad_scores = rounded(probabilities * (grad_probs - correction.T[..., None]))
    grad_query = jnp.einsum('hqk,khd->qhd', grad_scores, key_f) * scaling
    grad_key = jnp.einsum('hqk,qhd->khd', grad_scores, query_f) * scaling
    return (grad_query, grad_key, grad_value)

def reference(queries, key_vectors, value_vectors, grad_output):
    layout = (ROWS, ROW_LEN, HEADS, HEAD_DIM)
    query_rows = queries.reshape(layout)
    key_rows = key_vectors.reshape(layout)
    value_rows = value_vectors.reshape(layout)
    grad_rows = grad_output.reshape(layout)
    column_pos = jnp.arange(ROW_LEN)
    row_allowed = column_pos[None, :] <= column_pos[:, None]
    row_pos = jnp.arange(ROWS)
    column_allowed = row_pos[None, :] < row_pos[:, None]

    def swapped(array):
        return jnp.swapaxes(array, 0, 1)
    row_acc, row_max, row_tot = lax.map(lambda blocks: pattern_forward(blocks[0], blocks[1], blocks[2], row_allowed), (query_rows, key_rows, value_rows))
    col_acc, col_max, col_tot = lax.map(lambda blocks: pattern_forward(blocks[0], blocks[1], blocks[2], column_allowed), (swapped(query_rows), swapped(key_rows), swapped(value_rows)))
    col_acc, col_max, col_tot = (swapped(col_acc), swapped(col_max), swapped(col_tot))
    col_floor = jnp.maximum(col_tot, 1.0)
    col_out = rounded(col_acc / col_floor[..., None])
    col_lse = col_max + jnp.log(col_floor)
    maxima = jnp.maximum(row_max, col_lse)
    row_weight = jnp.exp(row_max - maxima)
    col_weight = jnp.exp(col_lse - maxima)
    denominators = row_tot * row_weight + col_weight
    attended = (row_acc * row_weight[..., None] + col_out * col_weight[..., None]) / denominators[..., None]
    log_totals = maxima + jnp.log(denominators)
    attended_low = attended.astype(jnp.bfloat16)
    correction = lax.optimization_barrier(jnp.sum(grad_rows.astype(jnp.float32) * lax.optimization_barrier(attended_low).astype(jnp.float32), axis=-1))
    row_grads = lax.map(lambda blocks: pattern_backward(blocks[0], blocks[1], blocks[2], blocks[3], blocks[4], blocks[5], row_allowed), (query_rows, key_rows, value_rows, grad_rows, log_totals, correction))
    col_grads = lax.map(lambda blocks: pattern_backward(blocks[0], blocks[1], blocks[2], blocks[3], blocks[4], blocks[5], column_allowed), (swapped(query_rows), swapped(key_rows), swapped(value_rows), swapped(grad_rows), swapped(log_totals), swapped(correction)))
    outputs = []
    for row_part, col_part in zip(row_grads, col_grads):
        total = row_part + rounded(swapped(col_part))
        outputs.append(total.astype(jnp.bfloat16).reshape(TOKENS, HEADS * HEAD_DIM))
    return (attended_low.reshape(TOKENS, HEADS * HEAD_DIM), outputs[0], outputs[1], outputs[2])
```

```python
import functools
import math

import jax
import jax.numpy as jnp
from jax import lax
from jax.experimental import pallas as pl
from jax.experimental.pallas import tpu as pltpu
from jax.sharding import PartitionSpec as P

ROW_LEN = 512
HEAD_DIM = 128
GROUP = 8
CHUNK = 256
PIECES = 2
MASKED = -1e30
FLOOR = -1e20
LOG2E = 1.0 / math.log(2.0)
SCALE = 1.0 / math.sqrt(HEAD_DIM)
F32 = jnp.float32
BF16 = jnp.bfloat16


def dot_t(left, right):
    return lax.dot_general(left, right, (((1,), (1,)), ((), ())), preferred_element_type=F32)


def dot_f(left, right):
    return lax.dot_general(left, right, (((0,), (0,)), ((), ())), preferred_element_type=F32)


def dot(left, right):
    return jnp.dot(left, right, preferred_element_type=F32)


def row_bias(first, key_chunk, query_chunk):
    if key_chunk < query_chunk:
        return None
    keys = lax.broadcasted_iota(jnp.int32, (CHUNK, CHUNK), 0)
    queries = lax.broadcasted_iota(jnp.int32, (CHUNK, CHUNK), 1)
    return jnp.where(keys <= queries, 0.0, MASKED)


def col_bias(first, key_chunk, query_chunk):
    keys = lax.broadcasted_iota(jnp.int32, (CHUNK, CHUNK), 0)
    queries = lax.broadcasted_iota(jnp.int32, (CHUNK, CHUNK), 1)
    gap = queries - keys
    same = (gap & (GROUP - 1)) == 0
    if key_chunk == query_chunk:
        same = same & (gap > 0)
    return jnp.where(same, 0.0, MASKED)


def chunk(array, index):
    return array[index * CHUNK : (index + 1) * CHUNK]


def scores_of(query, keys, bias, query_chunk):
    out = []
    for j in range(query_chunk + 1):
        s = dot_t(chunk(keys, j), query) * (SCALE * LOG2E)
        b = bias(None, j, query_chunk)
        out.append(s if b is None else s + b)
    return out


def softmax_of(scores, values):
    top = functools.reduce(
        jnp.maximum, [jnp.max(s, axis=0, keepdims=True) for s in scores]
    )
    top = jnp.maximum(top, FLOOR)
    weights = [jnp.exp2(s - top) for s in scores]
    total = sum(jnp.sum(w, axis=0, keepdims=True) for w in weights)
    acc = sum(dot_f(chunk(values, j), w.astype(BF16)) for j, w in enumerate(weights))
    total = jnp.maximum(total, 1.0)
    return weights, top, total, acc / total


def merge(left, right):
    top = jnp.maximum(left, right)
    w_left, w_right = jnp.exp2(left - top), jnp.exp2(right - top)
    den = w_left + w_right
    return top + jnp.log2(den), w_left / den, w_right / den


def backward_of(i, probs, delta, q, k, v, g, gk, gv):
    query, grad = chunk(q, i), chunk(g, i)
    gq = None
    for j, p in enumerate(probs):
        dv = dot(p.astype(BF16), grad)
        dp = dot_t(chunk(v, j), grad)
        ds = (p * (dp - delta)).astype(BF16)
        dk = dot(ds, query)
        dq = dot_f(chunk(k, j), ds)
        gv[j] = dv if gv[j] is None else gv[j] + dv
        gk[j] = dk if gk[j] is None else gk[j] + dk
        gq = dq if gq is None else gq + dq
    return (gq * SCALE).T


def row_forward_kernel(q_ref, k_ref, v_ref, g_ref, o_ref, lse_ref, dot_ref):
    q, k, v, g = q_ref[0], k_ref[0], v_ref[0], g_ref[0]
    for i in range(q.shape[0] // CHUNK):
        span = slice(i * CHUNK, (i + 1) * CHUNK)
        _, top, total, out = softmax_of(scores_of(chunk(q, i), k, row_bias, i), v)
        o_ref[0, 0, :, span] = out
        lse_ref[0, 0, :, span] = top + jnp.log2(total)
        grad_t = chunk(g, i).astype(F32).T
        dot_ref[0, 0, :, span] = jnp.sum(grad_t * out, axis=0, keepdims=True)


def row_forward(q, k, v, g):
    rows, length, width = q.shape
    heads = width // HEAD_DIM
    block = pl.BlockSpec((1, length, HEAD_DIM), lambda r, h: (r, 0, h))
    stat = pl.BlockSpec((1, 1, 1, length), lambda r, h: (r, h, 0, 0))
    stat_shape = jax.ShapeDtypeStruct((rows, heads, 1, length), F32)
    return pl.pallas_call(
        row_forward_kernel,
        grid=(rows, heads),
        in_specs=[block] * 4,
        out_specs=[
            pl.BlockSpec((1, 1, HEAD_DIM, length), lambda r, h: (r, h, 0, 0)),
            stat,
            stat,
        ],
        out_shape=[
            jax.ShapeDtypeStruct((rows, heads, HEAD_DIM, length), F32),
            stat_shape,
            stat_shape,
        ],
        cost_estimate=pl.CostEstimate(
            flops=rows * heads * length * length * HEAD_DIM * 8,
            bytes_accessed=rows * length * width * 12,
            transcendentals=rows * heads * length * length,
        ),
        name="row_forward",
    )(q, k, v, g)


def col_kernel(x_ref, stat_ref, y_ref, lse_ref):
    devices, _, _, per, width = x_ref.shape
    tokens = devices * per
    chunks = tokens // CHUNK
    q, k, v, g = [x_ref[:, a, 0].reshape(tokens, width) for a in range(4)]
    gk, gv = [None] * chunks, [None] * chunks
    slab = CHUNK // per
    for i in range(chunks):
        span = slice(i * CHUNK, (i + 1) * CHUNK)
        here = slice(i * slab, (i + 1) * slab)
        weights, top, total, out = softmax_of(scores_of(chunk(q, i), k, col_bias, i), v)
        lse_col = top + jnp.log2(total)
        lse_ref[0, 0, :, span] = lse_col
        out_low = out.T.astype(BF16)
        y_ref[here, 0, 0] = out_low.reshape(slab, per, width)
        lse, w_row, w_col = merge(stat_ref[0, 0, 0, :, span], lse_col)
        dot_col = jnp.sum(
            (chunk(g, i).astype(F32) * out_low.astype(F32)).T, axis=0, keepdims=True
        )
        delta = w_row * stat_ref[1, 0, 0, :, span] + w_col * dot_col
        factor = jnp.exp2(top - lse)
        probs = [w * factor for w in weights]
        gq = backward_of(i, probs, delta, q, k, v, g, gk, gv)
        y_ref[here, 1, 0] = gq.astype(BF16).reshape(slab, per, width)
    for j in range(chunks):
        here = slice(j * slab, (j + 1) * slab)
        y_ref[here, 2, 0] = (gk[j] * SCALE).astype(BF16).reshape(slab, per, width)
        y_ref[here, 3, 0] = gv[j].astype(BF16).reshape(slab, per, width)


def col_both(x, stats, first_head):
    devices, kinds, groups, per, width = x.shape
    heads = width // HEAD_DIM
    tokens = devices * per
    block = pl.BlockSpec(
        (devices, kinds, 1, per, HEAD_DIM), lambda c, h: (0, 0, c, 0, h)
    )
    return pl.pallas_call(
        col_kernel,
        grid=(groups, heads),
        in_specs=[
            block,
            pl.BlockSpec((2, 1, 1, 1, tokens), lambda c, h: (0, first_head + h, c, 0, 0)),
        ],
        out_specs=[block, pl.BlockSpec((1, 1, 1, tokens), lambda c, h: (h, c, 0, 0))],
        out_shape=[
            jax.ShapeDtypeStruct(x.shape, BF16),
            jax.ShapeDtypeStruct((heads, groups, 1, tokens), F32),
        ],
        cost_estimate=pl.CostEstimate(
            flops=groups * heads * tokens * tokens * HEAD_DIM * 20,
            bytes_accessed=x.size * 4,
            transcendentals=groups * heads * tokens * tokens,
        ),
        name="col_both",
    )(x, stats)


def row_backward_kernel(
    q_ref, k_ref, v_ref, g_ref, o_ref, lse_ref, back_ref, lse_col_ref, *rest
):
    att_ref, gq_ref, gk_ref, gv_ref = rest[-4:]
    q, k, v, g = q_ref[0], k_ref[0], v_ref[0], g_ref[0]
    length = q.shape[0]
    chunks = length // CHUNK
    devices = back_ref.shape[0]
    slab = devices // chunks

    def came_back(kind, i):
        part = back_ref[i * slab : (i + 1) * slab, kind, :, 0].astype(F32)
        return part.reshape(CHUNK, HEAD_DIM)

    gk, gv = [None] * chunks, [None] * chunks
    for i in range(chunks):
        span = slice(i * CHUNK, (i + 1) * CHUNK)
        lse, w_row, w_col = merge(lse_ref[0, 0, :, span], lse_col_ref[0, 0, :, span])
        col_t = came_back(0, i).T
        att_t = o_ref[0, 0, :, span] * w_row + col_t * w_col
        low = att_t.T.astype(BF16)
        att_ref[0, span, :] = low
        delta = jnp.sum(
            (chunk(g, i).astype(F32) * low.astype(F32)).T, axis=0, keepdims=True
        )
        scores = scores_of(chunk(q, i), k, row_bias, i)
        probs = [jnp.exp2(s - lse) for s in scores]
        gq = backward_of(i, probs, delta, q, k, v, g, gk, gv)
        gq_ref[0, span, :] = (gq + came_back(1, i)).astype(BF16)
    for j in range(chunks):
        span = slice(j * CHUNK, (j + 1) * CHUNK)
        gk_ref[0, span, :] = (gk[j] * SCALE + came_back(2, j)).astype(BF16)
        gv_ref[0, span, :] = (gv[j] + came_back(3, j)).astype(BF16)


def row_backward(q, k, v, g, o, lse, back, lse_col, first_head, earlier):
    rows, length, width = q.shape
    devices, kinds, groups, _, size, piece = back.shape
    heads = piece // HEAD_DIM
    block = pl.BlockSpec((1, length, HEAD_DIM), lambda r, h: (r, 0, first_head + h))
    stat = pl.BlockSpec((1, 1, 1, length), lambda r, h: (r, first_head + h, 0, 0))
    in_specs = [block] * 4 + [
        pl.BlockSpec((1, 1, HEAD_DIM, length), lambda r, h: (r, first_head + h, 0, 0)),
        stat,
        pl.BlockSpec(
            (devices, kinds, groups, 1, size, HEAD_DIM), lambda r, h: (0, 0, 0, r, 0, h)
        ),
        pl.BlockSpec((1, 1, 1, length), lambda r, h: (r, h, 0, 0)),
    ]
    aliases = {}
    if earlier:
        aliases = {len(in_specs) + n: n for n in range(4)}
        in_specs = in_specs + [pl.BlockSpec(memory_space=pl.ANY)] * 4
    return pl.pallas_call(
        row_backward_kernel,
        grid=(rows, heads),
        in_specs=in_specs,
        out_specs=[block] * 4,
        out_shape=[jax.ShapeDtypeStruct(q.shape, BF16)] * 4,
        input_output_aliases=aliases,
        cost_estimate=pl.CostEstimate(
            flops=rows * heads * length * length * HEAD_DIM * 14,
            bytes_accessed=rows * length * piece * 28,
            transcendentals=rows * heads * length * length,
        ),
        name="row_backward",
    )(q, k, v, g, o, lse, back, lse_col, *earlier)


def exchange(array):
    return lax.all_to_all(array, "seq", split_axis=0, concat_axis=0, tiled=True)


def on_device(queries, key_vectors, value_vectors, grad_output):
    devices = lax.axis_size("seq")
    rows = queries.shape[0] // ROW_LEN
    width = queries.shape[1]
    heads = width // HEAD_DIM
    groups = ROW_LEN // devices // GROUP
    per = rows * GROUP
    tokens = devices * per
    piece = width // PIECES
    piece_heads = piece // HEAD_DIM
    arrays = (queries, key_vectors, value_vectors, grad_output)
    by_row = [a.reshape(rows, ROW_LEN, width) for a in arrays]

    arrived = []
    for n in range(PIECES):
        parts = [
            jnp.transpose(
                a[:, n * piece : (n + 1) * piece].reshape(rows, devices, groups, GROUP, piece),
                (1, 2, 0, 3, 4),
            )
            for a in arrays
        ]
        packed = jnp.stack(parts, axis=1).reshape(devices, 4, groups, per, piece)
        arrived.append(exchange(packed))

    o, lse, dots = row_forward(*by_row)
    stats = jnp.stack([lse, dots]).reshape(2, rows, heads, devices, groups, GROUP)
    stats = jnp.transpose(stats, (3, 0, 2, 4, 1, 5)).reshape(devices, -1)
    stats = exchange(stats).reshape(devices, 2, heads, groups, per)
    stats = jnp.transpose(stats, (1, 2, 3, 0, 4)).reshape(2, heads, groups, 1, tokens)

    returned = []
    for n in range(PIECES):
        y, lse_col = col_both(arrived[n], stats, n * piece_heads)
        lse_col = jnp.transpose(
            lse_col.reshape(piece_heads, groups, devices, per), (2, 0, 1, 3)
        ).reshape(devices, -1)
        lse_back = exchange(lse_col).reshape(devices, piece_heads, groups, rows, GROUP)
        lse_back = jnp.transpose(lse_back, (3, 1, 0, 2, 4)).reshape(
            rows, piece_heads, 1, ROW_LEN
        )
        back = exchange(y).reshape(devices, 4, groups, rows, GROUP, piece)
        returned.append((back, lse_back))

    outs = ()
    for n in range(PIECES):
        back, lse_back = returned[n]
        outs = row_backward(*by_row, o, lse, back, lse_back, n * piece_heads, tuple(outs))
    return tuple(a.reshape(queries.shape) for a in outs)


def solution(mesh):
    spec = P("seq", "head")
    return jax.shard_map(
        on_device,
        mesh=mesh,
        in_specs=(spec,) * 4,
        out_specs=(spec,) * 4,
        check_vma=False,
    )
```
